32 devices in a mesh: groups: 2 (over y), chain: 4 (over z), samp: 4 (over x, core).
Axes of the slice: x: 2, y: 2, z: 4, core: 2. Of those that a mesh axis runs over, the one named last changes fastest.
Arguments:
- dosage: bfloat16 [16384, 4096], P('samp', ('groups', 'chain')), parts along dimension 1
- filter_mask: int32 [4096], P(('groups', 'chain')), parts along dimension 0, may hold values 0 or 1
- counts: int32 [8], P(('groups', 'chain')), parts along dimension 0, may hold values from 128 to 512, as said below
Outputs:
- ld_tiles: float32 [8, 512, 3, 512], P(('groups', 'chain'), 'samp'), parts along dimension 0
The draws below stay inside these ranges and needn't reach their ends.
There are 2 independent parts, one for each index of `groups`. The reference program is written for one: setup_inputs(seed, part) draws one part's arguments, and reference() takes and returns one part's arrays. A program takes and returns all parts, laid end to end along the dimension named above; each array names one. Nothing has to cross between parts.
Inputs may be any that keep to these rules, and one draw needn't show every extreme that they name: `counts`: every block but the last holds 512 live variants; the last holds from 128 to 512.
All inputs are finite; a program needn't handle non-finite values. No bound on the sum of `filter_mask` on one device may be relied on, other than what follows from the above.
Results may differ from the reference program's by a relative error of at most 0.0013.
Values may be sent and summed in bfloat16 or wider, within the bound.
A program may use at most 64 MiB of HBM per device.

```python
import jax
import jax.numpy as jnp
from jax import lax

BLK = 512
BAND = 3
BLOCKS = 4
VARIANTS = 2048
SAMPLES = 16384


def draw_dosage(key, part):
    keys = jax.random.split(jax.random.fold_in(key, 11), 4)
    place = jnp.arange(SAMPLES, dtype=jnp.float32) / SAMPLES
    row_scale = jnp.exp(jnp.log(10.0) * (0.5 * place + 0.5 * jax.random.uniform(keys[0], (SAMPLES,))))
    col_scale = jnp.exp(jnp.log(10.0) * jax.random.uniform(keys[1], (VARIANTS,)))
    centre = jax.random.uniform(keys[2], (VARIANTS,), minval=0.0, maxval=2.0)
    noise = jax.random.normal(keys[3], (SAMPLES, VARIANTS))
    mixed = noise + 0.6 * jnp.roll(noise, 1, axis=1) + 0.3 * jnp.roll(noise, 2, axis=1)
    values = centre[None, :] + 0.3 * mixed * row_scale[:, None] * col_scale[None, :]
    return values.astype(jnp.bfloat16)


def draw_counts(key, part):
    last = jax.random.randint(jax.random.fold_in(key, 23), (), BLK // 4, BLK + 1)
    index = jnp.arange(BLOCKS, dtype=jnp.int32)
    return jnp.where(index == BLOCKS - 1, last, BLK).astype(jnp.int32)


def with_ends(result, key, least, top_value):
    longest = result.shape.index(max(result.shape))
    spots = []
    for shift in (0, 1):
        where = [jax.random.randint(jax.random.fold_in(key, axis), (), 0, length) for axis, length in enumerate(result.shape)]
        where[longest] = (where[longest] + shift) % result.shape[longest]
        spots.append(tuple(where))
    return result.at[spots[0]].set(least).at[spots[1]].set(top_value)


def setup_inputs(seed: int = 0, part: int = 0) -> dict:
    arg_keys = jax.random.split(jax.random.key(seed), 4)
    own_keys = jax.random.split(jax.random.fold_in(arg_keys[3], part), 4)
    return {
        "dosage": draw_dosage(jax.random.fold_in(jax.random.fold_in(arg_keys[3], part), 71), part),
        "filter_mask": with_ends((jax.random.randint(own_keys[1], (VARIANTS,), 0, 8) < 7).astype(jnp.int32), jax.random.fold_in(own_keys[1], 1), 0, 1),
        "counts": draw_counts(jax.random.fold_in(jax.random.fold_in(arg_keys[3], part), 71), part),
    }


def reference(dosage, filter_mask, counts):
    samples = dosage.shape[0]
    values = dosage.astype(jnp.float32)
    mean = lax.optimization_barrier(jnp.sum(values, 0)) / samples
    var = lax.optimization_barrier(jnp.sum(values * values, 0)) / samples - mean * mean
    index = jnp.arange(VARIANTS, dtype=jnp.int32)
    inside = index % BLK
    owner = index // BLK
    live = (inside < counts[owner]).astype(jnp.float32)
    keep = filter_mask.astype(jnp.float32) * live
    scaled = ((values - mean) * lax.rsqrt(var + 1e-05) * keep).astype(jnp.bfloat16)
    padded = jnp.concatenate([scaled, jnp.zeros((samples, 2 * BLK), jnp.bfloat16)], axis=1)

    def one_block(block):
        start = (block * BLK).astype(jnp.int32)
        window = lax.dynamic_slice_in_dim(padded, start, BAND * BLK, 1)
        left = window[:, :BLK]
        tile = lax.dot_general(left, window, (((0,), (0,)), ((), ())), preferred_element_type=jnp.float32)
        return (tile / samples).reshape(BLK, BAND, BLK)
    return lax.map(one_block, jnp.arange(BLOCKS, dtype=jnp.int32))
```

```python
import functools

import jax
import jax.numpy as jnp
from jax import lax
from jax.experimental import pallas as pl
from jax.experimental.pallas import tpu as pltpu
from jax.sharding import PartitionSpec as P

MESH = pl.DeviceIdType.MESH
PARTS = 4
FINE = 4


def remote(src, dst, send_sem, recv_sem, where):
    return pltpu.make_async_remote_copy(
        src_ref=src, dst_ref=dst, send_sem=send_sem, recv_sem=recv_sem,
        device_id=where, device_id_type=MESH,
    )


def kernel(n, peers, samples, dosage, mask, counts, near,
           own, left, right, own_t, left_t, right_t,
           part0, part1, part2, pair0, pair1, pair2, far0, far1, far2,
           sums, stats, moments, left_moments, right_moments, total2, far,
           last1, last_rows, last_columns, out_rows, out_columns, land1, land_rows, land_columns,
           load_sem, send_z, recv_z, send_m, recv_m, send_s, recv_s,
           send_a, recv_a, send_b, recv_b, send_f, recv_f,
           send_1, recv_1, send_r, recv_r, send_c, recv_c):
    m = lax.axis_index("chain")
    me = lax.axis_index("samp")
    mine, odd = me // 2, me % 2
    rows, width = own.shape
    cut = width // peers
    deep = rows // PARTS
    coarse = width - cut
    fine = cut // FINE
    middle = width - fine
    has_left, has_right = m > 0, m < n - 1
    up, down = {"chain": m + 1}, {"chain": m - 1}

    load = pltpu.make_async_copy(dosage, own, load_sem)
    load.start()

    barrier = pltpu.get_barrier_semaphore()
    for r in range(peers):
        @pl.when(me != r)
        def _():
            pl.semaphore_signal(barrier, inc=1, device_id={"samp": r}, device_id_type=MESH)

    @pl.when(has_left)
    def _():
        pl.semaphore_signal(barrier, inc=1, device_id=down, device_id_type=MESH)

    @pl.when(has_right)
    def _():
        pl.semaphore_signal(barrier, inc=1, device_id=up, device_id_type=MESH)

    pl.semaphore_wait(barrier, peers - 1 + has_left.astype(jnp.int32) + has_right.astype(jnp.int32))

    def block_of(c, k):
        return pl.ds(pl.multiple_of(k * deep, deep), deep), pl.ds(c * cut, cut)

    def z_copy(way, c, k):
        at = block_of(c, k)
        return remote(dosage.at[at], (left, right)[way].at[at], send_z.at[way, c, k],
                      recv_z.at[way, c, k], (up, down)[way])

    slabs = ((coarse, cut - fine), (middle, fine))

    def t_copy(way, f, k):
        first, count = slabs[f]
        at = pl.ds(pl.multiple_of(k * deep, deep), deep)
        landing = (left_t.at[pl.ds(first, count), at], right_t.at[pl.ds(first - coarse, count), at])[way]
        return remote(own_t.at[pl.ds(first, count), at], landing, send_z.at[way, peers - 1 + f, k],
                      recv_z.at[way, peers - 1 + f, k], (up, down)[way])

    def m_copy(way):
        return remote(moments, (left_moments, right_moments)[way], send_m.at[way],
                      recv_m.at[way], (up, down)[way])

    def each_way(action):
        for way, present in ((0, has_right), (1, has_left)):
            @pl.when(present)
            def _():
                action(way)

    def start_z(c):
        def go(way):
            for k in range(PARTS):
                z_copy(way, c, k).start()
        each_way(go)

    def start_t(f):
        def go(way):
            for k in range(PARTS):
                t_copy(way, f, k).start()
        each_way(go)

    start_z(0)

    @pl.when(jnp.logical_not(has_left))
    def _():
        left[...] = jnp.zeros_like(left)
        left_t[coarse:, :] = jnp.zeros((cut, rows), left_t.dtype)
        left_moments[...] = jnp.zeros_like(left_moments)

    @pl.when(jnp.logical_not(has_right))
    def _():
        right[...] = jnp.zeros_like(right)
        right_t[...] = jnp.zeros_like(right_t)
        right_moments[...] = jnp.zeros_like(right_moments)

    part0[...] = jnp.zeros_like(part0)
    part1[...] = jnp.zeros_like(part1)
    part2[...] = jnp.zeros_like(part2)
    last1[...] = jnp.zeros_like(last1)
    last_rows[...] = jnp.zeros_like(last_rows)
    last_columns[...] = jnp.zeros_like(last_columns)
    load.wait()

    step = 64

    def add_up(i, carry):
        s, q = carry
        v = own[pl.ds(pl.multiple_of(i * step, step), step), :].astype(jnp.float32)
        v = v.reshape(step // 8, 8, width)
        return s + jnp.sum(v, 0), q + jnp.sum(v * v, 0)

    zero = jnp.zeros((8, width), jnp.float32)
    s, q = lax.fori_loop(0, rows // step, add_up, (zero, zero))
    sums[0:1, :] = jnp.sum(s, 0, keepdims=True)
    sums[1:2, :] = jnp.sum(q, 0, keepdims=True)

    def s_copy(r):
        return remote(sums, stats.at[me], send_s.at[r], recv_s.at[me], {"samp": r})

    def s_from(j):
        return remote(sums, stats.at[j], send_s.at[j], recv_s.at[j], {"samp": j})

    def others(action):
        for r in range(peers):
            @pl.when(me != r)
            def _():
                action(r)

    others(lambda r: s_copy(r).start())
    stats[me] = sums[...]
    others(lambda r: s_from(r).wait_recv())
    both = stats[0]
    for j in range(1, peers):
        both = both + stats[j]
    mean = both[0:1] / samples
    var = both[1:2] / samples - mean * mean
    live = (lax.broadcasted_iota(jnp.int32, (1, width), 1) < counts[0]).astype(jnp.float32)
    keep = mask[...].astype(jnp.float32) * live
    moments[0:1, :] = mean
    moments[1:2, :] = lax.rsqrt(var + 1e-05) * keep
    each_way(lambda way: m_copy(way).start())
    for c in range(1, peers - 1):
        start_z(c)

    def standard(ref, at, which):
        v = ref[at].astype(jnp.float32)
        return (v - which[0:1, at[1]]) * which[1:2, at[1]]

    parts, pairs, fars = (part0, part1, part2), (pair0, pair1, pair2), (far0, far1, far2)

    def pair_copy(kind, c, r):
        columns = columns_of(kind, c, r)
        return remote(
            parts[kind].at[pl.ds(r * cut, cut), columns], pairs[kind].at[r // 2, :, columns],
            send_a.at[kind, c, r // 2], recv_a.at[kind, c, r // 2], {"samp": me + 1 - 2 * odd})

    def far_copy(kind, c, r, source):
        columns = columns_of(kind, c, r)
        return remote(
            pairs[kind].at[r // 2, :, columns], fars[kind].at[source, :, columns],
            send_b.at[kind, c, r // 2], recv_b.at[kind, c, source], {"samp": r})

    def columns_of(kind, c, r):
        if kind == 0:
            return pl.ds(0, width)
        if kind == 1 or r < c:
            return pl.ds(c * cut, cut)
        return pl.ds(0, (c + 1) * cut)

    def takes(kind, c):
        return range(c + 1) if kind == 2 else range(peers)

    def send_pairs(kind, c, wait=False):
        for r in takes(kind, c):
            @pl.when(odd != r % 2)
            def _():
                copy = pair_copy(kind, c, r)
                copy.wait_send() if wait else copy.start()

    def sum_pairs(kind, c):
        for r in takes(kind, c):
            @pl.when(odd == r % 2)
            def _():
                columns = columns_of(kind, c, r)
                pair_copy(kind, c, r).wait_recv()
                pairs[kind][r // 2, :, columns] += parts[kind][pl.ds(r * cut, cut), columns]

                @pl.when(mine != r // 2)
                def _():
                    far_copy(kind, c, r, mine).start()

    def sent_pairs(kind, c):
        for r in takes(kind, c):
            @pl.when(jnp.logical_and(odd == r % 2, mine != r // 2))
            def _():
                far_copy(kind, c, r, mine).wait_send()

    def ship(columns, c):
        return remote(total2.at[:, columns], far.at[:, columns], send_f.at[c], recv_f.at[c], down)

    def collect(kind, c):
        for r in takes(kind, c):
            @pl.when(me == r)
            def _():
                columns = columns_of(kind, c, r)
                whole = pairs[kind][r // 2, :, columns]
                for q in range(peers // 2):
                    if q != r // 2:
                        far_copy(kind, c, r, q).wait_recv()
                        whole = whole + fars[kind][q, :, columns]
                if kind < 2:
                    near[kind, :, columns] = whole
                else:
                    total2[:, columns] = whole.astype(total2.dtype)

    def start_ship(c):
        for r in takes(2, c):
            @pl.when(jnp.logical_and(me == r, has_left))
            def _():
                ship(columns_of(2, c, r), c).start()

    def own_step(k, _):
        at = pl.ds(pl.multiple_of(k * deep, deep), deep)
        for c in range(peers):
            here = (at, pl.ds(c * cut, cut))
            z = standard(own, here, moments)
            own[here] = z.astype(jnp.bfloat16)
            own_t[pl.ds(c * cut, cut), at] = z.T.astype(jnp.bfloat16)
        part0[...] += jnp.dot(own_t[:, at], own[at, :], preferred_element_type=jnp.float32)
        return 0

    lax.fori_loop(0, PARTS, own_step, 0)
    send_pairs(0, 0)

    def wait_moments(way):
        m_copy(1 - way).wait_recv()

    each_way(wait_moments)

    def across(a, b):
        return lax.dot_general(a, b, (((1,), (1,)), ((), ())), preferred_element_type=jnp.float32)

    def along(a, b):
        return jnp.dot(a, b, preferred_element_type=jnp.float32)

    for c in range(peers - 1):
        def one(k, _, c=c):
            at, columns = here = block_of(c, k)
            earlier = ((2, c - 1), (1, c - 1)) if c else ((0, 0),)

            @pl.when(k == 1)
            def _():
                for which in earlier:
                    sum_pairs(*which)

            @pl.when(k == PARTS - 1)
            def _():
                for which in earlier:
                    collect(*which)

            @pl.when(has_left)
            def _():
                z_copy(0, c, k).wait_recv()

            z = standard(left, here, left_moments)
            left[here] = z.astype(jnp.bfloat16)
            left_t[columns, at] = z.T.astype(jnp.bfloat16)

            @pl.when(has_right)
            def _():
                z_copy(1, c, k).wait_recv()

            right[here] = standard(right, here, right_moments).astype(jnp.bfloat16)
            part1[:, columns] += along(own_t[:, at], right[here])
            top = pl.ds(0, (c + 1) * cut)
            part2[top, columns] += along(left_t[top, at], right[here])
            if c:
                front = pl.ds(0, c * cut)
                part2[columns, front] += along(left_t[columns, at], right[at, front])
            return 0

        lax.fori_loop(0, PARTS, one, 0)
        send_pairs(2, c)
        send_pairs(1, c)
        if c == 0:
            start_t(0)

    def wait_slab(f, k):
        @pl.when(has_left)
        def _():
            t_copy(0, f, k).wait_recv()

        @pl.when(has_right)
        def _():
            t_copy(1, f, k).wait_recv()

    whole_front, slab = pl.ds(0, coarse), pl.ds(coarse, cut - fine)

    def first_slab(k, _):
        at = pl.ds(pl.multiple_of(k * deep, deep), deep)

        @pl.when(k == 1)
        def _():
            sum_pairs(2, peers - 2)
            sum_pairs(1, peers - 2)

        @pl.when(k == 2)
        def _():
            collect(2, peers - 2)
            for c in range(peers - 1):
                start_ship(c)
            start_t(1)
            collect(1, peers - 2)

        wait_slab(0, k)
        new = right_t[pl.ds(0, cut - fine), at]
        part1[:, slab] += across(own_t[:, at], new)
        part2[pl.ds(0, middle), slab] += across(left_t[pl.ds(0, middle), at], new)
        part2[slab, whole_front] += along(left_t[slab, at], right[at, :])
        return 0

    lax.fori_loop(0, PARTS, first_slab, 0)
    send_pairs(2, peers - 1)
    send_pairs(1, peers - 1)
    sum_pairs(2, peers - 1)
    sum_pairs(1, peers - 1)

    def last_slab(k, _):
        at = pl.ds(pl.multiple_of(k * deep, deep), deep)
        wait_slab(1, k)
        new = right_t[pl.ds(cut - fine, fine), at]
        last_columns[:, whole_front] += along(new, left[at, :])
        last_columns[:, slab] += across(new, left_t[slab, at])
        new_left = left_t[pl.ds(middle, fine), at]
        last_rows[:, whole_front] += along(new_left, right[at, :])
        last_rows[:, pl.ds(coarse, cut)] += across(new_left, right_t[:, at])
        last1[...] += along(new, own[at, :])
        return 0

    lax.fori_loop(0, PARTS, last_slab, 0)

    def columns_copy(r, source):
        return remote(out_columns.at[:, pl.ds(r * cut, cut)], land_columns.at[source],
                      send_c.at[r], recv_c.at[source], {"chain": m - 1, "samp": r})

    def rows_copy(source):
        return remote(out_rows, land_rows.at[source], send_r, recv_r.at[source],
                      {"chain": m - 1, "samp": peers - 1})

    def last1_copy(r, source):
        return remote(last1.at[:, pl.ds(r * cut, cut)], land1.at[source],
                      send_1.at[r], recv_1.at[source], {"samp": r})

    out_columns[...] = last_columns[...].astype(out_columns.dtype)
    out_rows[...] = last_rows[...].astype(out_rows.dtype)

    @pl.when(has_left)
    def _():
        rows_copy(me).start()
        for r in range(peers):
            columns_copy(r, me).start()

    others(lambda r: last1_copy(r, me).start())
    for r in range(peers):
        @pl.when(me == r)
        def _():
            land1[r] = last1[:, pl.ds(r * cut, cut)]

    collect(2, peers - 1)
    start_ship(peers - 1)
    collect(1, peers - 1)

    def turned(landed):
        total = landed[0].astype(jnp.float32)
        for j in range(1, peers):
            total = total + landed[j].astype(jnp.float32)
        return jnp.concatenate([jnp.zeros((cut - fine, cut), jnp.float32), total], 0).T

    others(lambda r: last1_copy(r, r).wait_recv())
    near[1, :, pl.ds(coarse, cut)] += turned(land1)

    @pl.when(jnp.logical_not(has_right))
    def _():
        near[2] = jnp.zeros_like(near[2])

    @pl.when(has_right)
    def _():
        for c in range(peers):
            for r in takes(2, c):
                @pl.when(me == r)
                def _():
                    ship(columns_of(2, c, r), c).wait_recv()
        near[2] = far[...].astype(jnp.float32)
        for source in range(peers):
            columns_copy(0, source).wait_recv()
        near[2, :, pl.ds(coarse, cut)] += turned(land_columns)

        @pl.when(me == peers - 1)
        def _():
            total = jnp.zeros((fine, width), jnp.float32)
            for source in range(peers):
                rows_copy(source).wait_recv()
                total = total + land_rows[source].astype(jnp.float32)
            near[2, pl.ds(cut - fine, fine), :] += total

    @pl.when(has_left)
    def _():
        rows_copy(me).wait_send()
        for r in range(peers):
            columns_copy(r, me).wait_send()

    others(lambda r: last1_copy(r, me).wait_send())
    others(lambda r: s_copy(r).wait_send())
    each_way(lambda way: m_copy(way).wait_send())

    def sent(way):
        for k in range(PARTS):
            for c in range(peers - 1):
                z_copy(way, c, k).wait_send()
            for f in range(2):
                t_copy(way, f, k).wait_send()

    each_way(sent)
    for c in range(peers):
        for kind in (1, 2):
            send_pairs(kind, c, True)
            sent_pairs(kind, c)
        for r in takes(2, c):
            @pl.when(jnp.logical_and(me == r, has_left))
            def _():
                ship(columns_of(2, c, r), c).wait_send()
    send_pairs(0, 0, True)
    sent_pairs(0, 0)


def body(n, peers, dosage, filter_mask, counts):
    rows, width = dosage.shape
    cut = width // peers
    fine = cut // FINE
    samples = rows * peers
    f32, bf16 = jnp.float32, jnp.bfloat16
    vmem = pl.BlockSpec(memory_space=pltpu.VMEM)
    dma = pltpu.SemaphoreType.DMA
    tiles = pl.pallas_call(
        functools.partial(kernel, n, peers, samples),
        out_shape=jax.ShapeDtypeStruct((3, cut, width), f32),
        in_specs=[pl.BlockSpec(memory_space=pl.ANY), vmem, pl.BlockSpec(memory_space=pltpu.SMEM)],
        out_specs=vmem,
        scratch_shapes=[
            pltpu.VMEM((rows, width), bf16),
            *[pltpu.VMEM((rows, width - cut), bf16)] * 2,
            *[pltpu.VMEM((width, rows), bf16)] * 2,
            pltpu.VMEM((cut, rows), bf16),
            *[pltpu.VMEM((width, width), f32)] * 3,
            *[pltpu.VMEM((peers // 2, cut, width), f32)] * 6,
            pltpu.VMEM((2, width), f32),
            pltpu.VMEM((peers, 2, width), f32),
            *[pltpu.VMEM((2, width), f32)] * 3,
            *[pltpu.VMEM((cut, width), bf16)] * 2,
            *[pltpu.VMEM((fine, width), f32)] * 3,
            *[pltpu.VMEM((fine, width), bf16)] * 2,
            pltpu.VMEM((peers, fine, cut), f32),
            pltpu.VMEM((peers, fine, width), bf16),
            pltpu.VMEM((peers, fine, cut), bf16),
            dma,
            *[dma((2, peers + 1, PARTS))] * 2,
            *[dma((2,))] * 2,
            *[dma((peers,))] * 2,
            *[dma((3, peers, peers // 2))] * 4,
            *[dma((peers,))] * 2,
            *[dma((peers,))] * 2,
            dma, dma((peers,)),
            *[dma((peers,))] * 2,
        ],
        compiler_params=pltpu.CompilerParams(
            collective_id=0, has_side_effects=True, vmem_limit_bytes=52 * 2**20),
    )(dosage, filter_mask[None], counts)
    return jnp.transpose(tiles / samples, (1, 0, 2))[None]


def solution(mesh):
    in_specs = (P("samp", ("groups", "chain")), P(("groups", "chain")), P(("groups", "chain")))
    out_specs = P(("groups", "chain"), "samp", None, None)
    run = functools.partial(body, mesh.shape["chain"], mesh.shape["samp"])
    return jax.shard_map(run, mesh=mesh, in_specs=in_specs, out_specs=out_specs, check_vma=False)
```

```python
import functools

import jax
import jax.numpy as jnp
from jax import lax
from jax.experimental import pallas as pl
from jax.experimental.pallas import tpu as pltpu
from jax.sharding import PartitionSpec as P

MESH = pl.DeviceIdType.MESH
PARTS = 4
FINE = 4


def remote(src, dst, send_sem, recv_sem, where):
    return pltpu.make_async_remote_copy(
        src_ref=src, dst_ref=dst, send_sem=send_sem, recv_sem=recv_sem,
        device_id=where, device_id_type=MESH,
    )


def kernel(n, peers, samples, dosage, filter_mask, block_counts, near,
           own, left, right, own_t, left_t, right_t,
           part0, part1, part2, pair0, pair1, pair2, far0, far1, far2,
           sums, stats, moments, left_moments, right_moments, total2, far,
           last1, last_rows, last_columns, out_rows, out_columns, land1, land_rows, land_columns,
           mask, counts, mask_sem, counts_sem, load_sem, send_z, recv_z, send_m, recv_m, send_s, recv_s,
           send_a, recv_a, send_b, recv_b, send_f, recv_f,
           send_1, recv_1, send_r, recv_r, send_c, recv_c):
    m = lax.axis_index("chain")
    me = lax.axis_index("samp")
    mine, odd = me // 2, me % 2
    rows, width = own.shape
    cut = width // peers
    deep = rows // PARTS
    coarse = width - cut
    fine = cut // FINE
    middle = width - fine
    has_left, has_right = m > 0, m < n - 1
    up, down = {"chain": m + 1}, {"chain": m - 1}

    load = pltpu.make_async_copy(dosage, own, load_sem)
    load.start()
    small = (pltpu.make_async_copy(filter_mask, mask, mask_sem), pltpu.make_async_copy(block_counts, counts, counts_sem))
    for copy in small:
        copy.start()

    barrier = pltpu.get_barrier_semaphore()
    for r in range(peers):
        @pl.when(me != r)
        def _():
            pl.semaphore_signal(barrier, inc=1, device_id={"samp": r}, device_id_type=MESH)

    @pl.when(has_left)
    def _():
        pl.semaphore_signal(barrier, inc=1, device_id=down, device_id_type=MESH)

    @pl.when(has_right)
    def _():
        pl.semaphore_signal(barrier, inc=1, device_id=up, device_id_type=MESH)

    pl.semaphore_wait(barrier, peers - 1 + has_left.astype(jnp.int32) + has_right.astype(jnp.int32))

    def block_of(c, k):
        return pl.ds(pl.multiple_of(k * deep, deep), deep), pl.ds(c * cut, cut)

    def z_copy(way, c, k):
        at = block_of(c, k)
        return remote(dosage.at[at], (left, right)[way].at[at], send_z.at[way, c, k],
                      recv_z.at[way, c, k], (up, down)[way])

    slabs = ((coarse, cut - fine), (middle, fine))

    def t_copy(way, f, k):
        first, count = slabs[f]
        at = pl.ds(pl.multiple_of(k * deep, deep), deep)
        landing = (left_t.at[pl.ds(first, count), at], right_t.at[pl.ds(first - coarse, count), at])[way]
        return remote(own_t.at[pl.ds(first, count), at], landing, send_z.at[way, peers - 1 + f, k],
                      recv_z.at[way, peers - 1 + f, k], (up, down)[way])

    def m_copy(way):
        return remote(moments, (left_moments, right_moments)[way], send_m.at[way],
                      recv_m.at[way], (up, down)[way])

    def each_way(action):
        for way, present in ((0, has_right), (1, has_left)):
            @pl.when(present)
            def _():
                action(way)

    def start_z(c):
        def go(way):
            for k in range(PARTS):
                z_copy(way, c, k).start()
        each_way(go)

    def start_t(f):
        def go(way):
            for k in range(PARTS):
                t_copy(way, f, k).start()
        each_way(go)

    start_z(0)

    @pl.when(jnp.logical_not(has_left))
    def _():
        left[...] = jnp.zeros_like(left)
        left_t[coarse:, :] = jnp.zeros((cut, rows), left_t.dtype)
        left_moments[...] = jnp.zeros_like(left_moments)

    @pl.when(jnp.logical_not(has_right))
    def _():
        right[...] = jnp.zeros_like(right)
        right_t[...] = jnp.zeros_like(right_t)
        right_moments[...] = jnp.zeros_like(right_moments)

    part0[...] = jnp.zeros_like(part0)
    part1[...] = jnp.zeros_like(part1)
    part2[...] = jnp.zeros_like(part2)
    last1[...] = jnp.zeros_like(last1)
    last_rows[...] = jnp.zeros_like(last_rows)
    last_columns[...] = jnp.zeros_like(last_columns)
    load.wait()

    step = 64

    def add_up(i, carry):
        s, q = carry
        v = own[pl.ds(pl.multiple_of(i * step, step), step), :].astype(jnp.float32)
        v = v.reshape(step // 8, 8, width)
        return s + jnp.sum(v, 0), q + jnp.sum(v * v, 0)

    zero = jnp.zeros((8, width), jnp.float32)
    s, q = lax.fori_loop(0, rows // step, add_up, (zero, zero))
    sums[0:1, :] = jnp.sum(s, 0, keepdims=True)
    sums[1:2, :] = jnp.sum(q, 0, keepdims=True)

    def s_copy(r):
        return remote(sums, stats.at[me], send_s.at[r], recv_s.at[me], {"samp": r})

    def s_from(j):
        return remote(sums, stats.at[j], send_s.at[j], recv_s.at[j], {"samp": j})

    def others(action):
        for r in range(peers):
            @pl.when(me != r)
            def _():
                action(r)

    others(lambda r: s_copy(r).start())
    stats[me] = sums[...]
    for copy in small:
        copy.wait()
    others(lambda r: s_from(r).wait_recv())
    both = stats[0]
    for j in range(1, peers):
        both = both + stats[j]
    mean = both[0:1] / samples
    var = both[1:2] / samples - mean * mean
    live = (lax.broadcasted_iota(jnp.int32, (1, width), 1) < counts[0]).astype(jnp.float32)
    keep = mask[...].astype(jnp.float32) * live
    moments[0:1, :] = mean
    moments[1:2, :] = lax.rsqrt(var + 1e-05) * keep
    each_way(lambda way: m_copy(way).start())
    for c in range(1, peers - 1):
        start_z(c)

    def standard(ref, at, which):
        v = ref[at].astype(jnp.float32)
        return (v - which[0:1, at[1]]) * which[1:2, at[1]]

    parts, pairs, fars = (part0, part1, part2), (pair0, pair1, pair2), (far0, far1, far2)

    def pair_copy(kind, c, r):
        columns = columns_of(kind, c, r)
        return remote(
            parts[kind].at[pl.ds(r * cut, cut), columns], pairs[kind].at[r // 2, :, columns],
            send_a.at[kind, c, r // 2], recv_a.at[kind, c, r // 2], {"samp": me + 1 - 2 * odd})

    def far_copy(kind, c, r, source):
        columns = columns_of(kind, c, r)
        return remote(
            pairs[kind].at[r // 2, :, columns], fars[kind].at[source, :, columns],
            send_b.at[kind, c, r // 2], recv_b.at[kind, c, source], {"samp": r})

    def columns_of(kind, c, r):
        if kind == 0:
            return pl.ds(0, width)
        if kind == 1 or r < c:
            return pl.ds(c * cut, cut)
        return pl.ds(0, (c + 1) * cut)

    def takes(kind, c):
        return range(c + 1) if kind == 2 else range(peers)

    def send_pairs(kind, c, wait=False):
        for r in takes(kind, c):
            @pl.when(odd != r % 2)
            def _():
                copy = pair_copy(kind, c, r)
                copy.wait_send() if wait else copy.start()

    def sum_pairs(kind, c):
        for r in takes(kind, c):
            @pl.when(odd == r % 2)
            def _():
                columns = columns_of(kind, c, r)
                pair_copy(kind, c, r).wait_recv()
                pairs[kind][r // 2, :, columns] += parts[kind][pl.ds(r * cut, cut), columns]

                @pl.when(mine != r // 2)
                def _():
                    far_copy(kind, c, r, mine).start()

    def sent_pairs(kind, c):
        for r in takes(kind, c):
            @pl.when(jnp.logical_and(odd == r % 2, mine != r // 2))
            def _():
                far_copy(kind, c, r, mine).wait_send()

    def ship(columns, c):
        return remote(total2.at[:, columns], far.at[:, columns], send_f.at[c], recv_f.at[c], down)

    def collect(kind, c):
        for r in takes(kind, c):
            @pl.when(me == r)
            def _():
                columns = columns_of(kind, c, r)
                whole = pairs[kind][r // 2, :, columns]
                for q in range(peers // 2):
                    if q != r // 2:
                        far_copy(kind, c, r, q).wait_recv()
                        whole = whole + fars[kind][q, :, columns]
                if kind < 2:
                    near[kind, :, columns] = whole
                else:
                    total2[:, columns] = whole.astype(total2.dtype)

    def start_ship(c):
        for r in takes(2, c):
            @pl.when(jnp.logical_and(me == r, has_left))
            def _():
                ship(columns_of(2, c, r), c).start()

    def own_step(k, _):
        at = pl.ds(pl.multiple_of(k * deep, deep), deep)
        for c in range(peers):
            here = (at, pl.ds(c * cut, cut))
            z = standard(own, here, moments)
            own[here] = z.astype(jnp.bfloat16)
            own_t[pl.ds(c * cut, cut), at] = z.T.astype(jnp.bfloat16)
        part0[...] += jnp.dot(own_t[:, at], own[at, :], preferred_element_type=jnp.float32)
        return 0

    lax.fori_loop(0, PARTS, own_step, 0)
    send_pairs(0, 0)

    def wait_moments(way):
        m_copy(1 - way).wait_recv()

    each_way(wait_moments)

    def across(a, b):
        return lax.dot_general(a, b, (((1,), (1,)), ((), ())), preferred_element_type=jnp.float32)

    def along(a, b):
        return jnp.dot(a, b, preferred_element_type=jnp.float32)

    for c in range(peers - 1):
        def one(k, _, c=c):
            at, columns = here = block_of(c, k)
            earlier = ((2, c - 1), (1, c - 1)) if c else ((0, 0),)

            @pl.when(k == 1)
            def _():
                for which in earlier:
                    sum_pairs(*which)

            @pl.when(k == PARTS - 1)
            def _():
                for which in earlier:
                    collect(*which)

            @pl.when(has_left)
            def _():
                z_copy(0, c, k).wait_recv()

            z = standard(left, here, left_moments)
            left[here] = z.astype(jnp.bfloat16)
            left_t[columns, at] = z.T.astype(jnp.bfloat16)

            @pl.when(has_right)
            def _():
                z_copy(1, c, k).wait_recv()

            right[here] = standard(right, here, right_moments).astype(jnp.bfloat16)
            part1[:, columns] += along(own_t[:, at], right[here])
            top = pl.ds(0, (c + 1) * cut)
            part2[top, columns] += along(left_t[top, at], right[here])
            if c:
                front = pl.ds(0, c * cut)
                part2[columns, front] += along(left_t[columns, at], right[at, front])
            return 0

        lax.fori_loop(0, PARTS, one, 0)
        send_pairs(2, c)
        send_pairs(1, c)
        if c == 0:
            start_t(0)
            start_t(1)

    def wait_slab(f, k):
        @pl.when(has_left)
        def _():
            t_copy(0, f, k).wait_recv()

        @pl.when(has_right)
        def _():
            t_copy(1, f, k).wait_recv()

    whole_front, slab = pl.ds(0, coarse), pl.ds(coarse, cut - fine)

    def first_slab(k, _):
        at = pl.ds(pl.multiple_of(k * deep, deep), deep)

        @pl.when(k == 1)
        def _():
            sum_pairs(2, peers - 2)
            sum_pairs(1, peers - 2)

        @pl.when(k == 2)
        def _():
            collect(2, peers - 2)
            for c in range(peers - 1):
                start_ship(c)
            collect(1, peers - 2)

        wait_slab(0, k)
        new = right_t[pl.ds(0, cut - fine), at]
        part1[:, slab] += across(own_t[:, at], new)
        part2[pl.ds(0, middle), slab] += across(left_t[pl.ds(0, middle), at], new)
        part2[slab, whole_front] += along(left_t[slab, at], right[at, :])
        return 0

    lax.fori_loop(0, PARTS, first_slab, 0)
    send_pairs(2, peers - 1)
    send_pairs(1, peers - 1)
    sum_pairs(2, peers - 1)
    sum_pairs(1, peers - 1)

    def last_slab(k, _):
        at = pl.ds(pl.multiple_of(k * deep, deep), deep)
        wait_slab(1, k)
        new = right_t[pl.ds(cut - fine, fine), at]
        last_columns[:, whole_front] += along(new, left[at, :])
        last_columns[:, slab] += across(new, left_t[slab, at])
        new_left = left_t[pl.ds(middle, fine), at]
        last_rows[:, whole_front] += along(new_left, right[at, :])
        last_rows[:, pl.ds(coarse, cut)] += across(new_left, right_t[:, at])
        last1[...] += along(new, own[at, :])
        return 0

    lax.fori_loop(0, PARTS, last_slab, 0)

    def columns_copy(r, source):
        return remote(out_columns.at[:, pl.ds(r * cut, cut)], land_columns.at[source],
                      send_c.at[r], recv_c.at[source], {"chain": m - 1, "samp": r})

    def rows_copy(source):
        return remote(out_rows, land_rows.at[source], send_r, recv_r.at[source],
                      {"chain": m - 1, "samp": peers - 1})

    def last1_copy(r, source):
        return remote(last1.at[:, pl.ds(r * cut, cut)], land1.at[source],
                      send_1.at[r], recv_1.at[source], {"samp": r})

    out_columns[...] = last_columns[...].astype(out_columns.dtype)
    out_rows[...] = last_rows[...].astype(out_rows.dtype)

    @pl.when(has_left)
    def _():
        rows_copy(me).start()
        for r in range(peers):
            columns_copy(r, me).start()

    others(lambda r: last1_copy(r, me).start())
    for r in range(peers):
        @pl.when(me == r)
        def _():
            land1[r] = last1[:, pl.ds(r * cut, cut)]

    collect(2, peers - 1)
    start_ship(peers - 1)
    collect(1, peers - 1)

    def turned(landed):
        total = landed[0].astype(jnp.float32)
        for j in range(1, peers):
            total = total + landed[j].astype(jnp.float32)
        return jnp.concatenate([jnp.zeros((cut - fine, cut), jnp.float32), total], 0).T

    others(lambda r: last1_copy(r, r).wait_recv())
    near[1, :, pl.ds(coarse, cut)] += turned(land1)

    @pl.when(jnp.logical_not(has_right))
    def _():
        near[2] = jnp.zeros_like(near[2])

    @pl.when(has_right)
    def _():
        for c in range(peers):
            for r in takes(2, c):
                @pl.when(me == r)
                def _():
                    ship(columns_of(2, c, r), c).wait_recv()
        near[2] = far[...].astype(jnp.float32)
        for source in range(peers):
            columns_copy(0, source).wait_recv()
        near[2, :, pl.ds(coarse, cut)] += turned(land_columns)

        @pl.when(me == peers - 1)
        def _():
            total = jnp.zeros((fine, width), jnp.float32)
            for source in range(peers):
                rows_copy(source).wait_recv()
                total = total + land_rows[source].astype(jnp.float32)
            near[2, pl.ds(cut - fine, fine), :] += total

    @pl.when(has_left)
    def _():
        rows_copy(me).wait_send()
        for r in range(peers):
            columns_copy(r, me).wait_send()

    others(lambda r: last1_copy(r, me).wait_send())
    others(lambda r: s_copy(r).wait_send())
    each_way(lambda way: m_copy(way).wait_send())

    def sent(way):
        for k in range(PARTS):
            for c in range(peers - 1):
                z_copy(way, c, k).wait_send()
            for f in range(2):
                t_copy(way, f, k).wait_send()

    each_way(sent)
    for c in range(peers):
        for kind in (1, 2):
            send_pairs(kind, c, True)
            sent_pairs(kind, c)
        for r in takes(2, c):
            @pl.when(jnp.logical_and(me == r, has_left))
            def _():
                ship(columns_of(2, c, r), c).wait_send()
    send_pairs(0, 0, True)
    sent_pairs(0, 0)


def body(n, peers, dosage, filter_mask, counts):
    rows, width = dosage.shape
    cut = width // peers
    fine = cut // FINE
    samples = rows * peers
    f32, bf16 = jnp.float32, jnp.bfloat16
    vmem = pl.BlockSpec(memory_space=pltpu.VMEM)
    dma = pltpu.SemaphoreType.DMA
    tiles = pl.pallas_call(
        functools.partial(kernel, n, peers, samples),
        out_shape=jax.ShapeDtypeStruct((3, cut, width), f32),
        in_specs=[pl.BlockSpec(memory_space=pl.ANY)] * 3,
        out_specs=vmem,
        scratch_shapes=[
            pltpu.VMEM((rows, width), bf16),
            *[pltpu.VMEM((rows, width - cut), bf16)] * 2,
            *[pltpu.VMEM((width, rows), bf16)] * 2,
            pltpu.VMEM((cut, rows), bf16),
            *[pltpu.VMEM((width, width), f32)] * 3,
            *[pltpu.VMEM((peers // 2, cut, width), f32)] * 6,
            pltpu.VMEM((2, width), f32),
            pltpu.VMEM((peers, 2, width), f32),
            *[pltpu.VMEM((2, width), f32)] * 3,
            *[pltpu.VMEM((cut, width), bf16)] * 2,
            *[pltpu.VMEM((fine, width), f32)] * 3,
            *[pltpu.VMEM((fine, width), bf16)] * 2,
            pltpu.VMEM((peers, fine, cut), f32),
            pltpu.VMEM((peers, fine, width), bf16),
            pltpu.VMEM((peers, fine, cut), bf16),
            pltpu.VMEM((1, width), jnp.int32),
            pltpu.SMEM((1,), jnp.int32),
            *[dma] * 3,
            *[dma((2, peers + 1, PARTS))] * 2,
            *[dma((2,))] * 2,
            *[dma((peers,))] * 2,
            *[dma((3, peers, peers // 2))] * 4,
            *[dma((peers,))] * 2,
            *[dma((peers,))] * 2,
            dma, dma((peers,)),
            *[dma((peers,))] * 2,
        ],
        compiler_params=pltpu.CompilerParams(
            collective_id=0, has_side_effects=True, vmem_limit_bytes=52 * 2**20),
    )(dosage, pltpu.with_memory_space_constraint(filter_mask[None], pltpu.HBM), counts)
    return jnp.transpose(tiles / samples, (1, 0, 2))[None]


def solution(mesh):
    in_specs = (P("samp", ("groups", "chain")), P(("groups", "chain")), P(("groups", "chain")))
    out_specs = P(("groups", "chain"), "samp", None, None)
    run = functools.partial(body, mesh.shape["chain"], mesh.shape["samp"])
    return jax.shard_map(run, mesh=mesh, in_specs=in_specs, out_specs=out_specs, check_vma=False)
```

```python
import functools

import jax
import jax.numpy as jnp
from jax import lax
from jax.experimental import pallas as pl
from jax.experimental.pallas import tpu as pltpu
from jax.sharding import PartitionSpec as P

MESH = pl.DeviceIdType.MESH
PARTS = 4
LAST_PARTS = 2
FINE = 4


def remote(src, dst, send_sem, recv_sem, where):
    return pltpu.make_async_remote_copy(
        src_ref=src, dst_ref=dst, send_sem=send_sem, recv_sem=recv_sem,
        device_id=where, device_id_type=MESH,
    )


def kernel(n, peers, samples, dosage, filter_mask, block_counts, near,
           own, left, right, own_t, left_t, right_t,
           part0, part1, part2, pair0, pair1, pair2, far0, far1, far2,
           sums, stats, moments, left_moments, right_moments, total2, far,
           last1, last_rows, last_columns, out_rows, out_columns, land1, land_rows, land_columns,
           mask, counts, mask_sem, counts_sem, load_sem, send_z, recv_z, send_m, recv_m, send_s, recv_s,
           send_a, recv_a, send_b, recv_b, send_f, recv_f,
           send_1, recv_1, send_r, recv_r, send_c, recv_c):
    m = lax.axis_index("chain")
    me = lax.axis_index("samp")
    mine, odd = me // 2, me % 2
    rows, width = own.shape
    cut = width // peers
    deep = rows // PARTS
    coarse = width - cut
    fine = cut // FINE
    middle = width - fine
    has_left, has_right = m > 0, m < n - 1
    up, down = {"chain": m + 1}, {"chain": m - 1}

    barrier = pltpu.get_barrier_semaphore()
    for r in range(peers):
        @pl.when(me != r)
        def _():
            pl.semaphore_signal(barrier, inc=1, device_id={"samp": r}, device_id_type=MESH)

    @pl.when(has_left)
    def _():
        pl.semaphore_signal(barrier, inc=1, device_id=down, device_id_type=MESH)

    @pl.when(has_right)
    def _():
        pl.semaphore_signal(barrier, inc=1, device_id=up, device_id_type=MESH)

    load = pltpu.make_async_copy(dosage, own, load_sem)
    load.start()
    small = (pltpu.make_async_copy(filter_mask, mask, mask_sem), pltpu.make_async_copy(block_counts, counts, counts_sem))
    for copy in small:
        copy.start()

    pl.semaphore_wait(barrier, peers - 1 + has_left.astype(jnp.int32) + has_right.astype(jnp.int32))

    def block_of(c, k):
        return pl.ds(pl.multiple_of(k * deep, deep), deep), pl.ds(c * cut, cut)

    def z_copy(way, c, k):
        at = block_of(c, k)
        return remote(dosage.at[at], (left, right)[way].at[at], send_z.at[way, c, k],
                      recv_z.at[way, c, k], (up, down)[way])

    slabs = ((coarse, cut - fine, PARTS), (middle, fine, LAST_PARTS))

    def piece(f, k):
        size = rows // slabs[f][2]
        return pl.ds(pl.multiple_of(k * size, size), size)

    def t_copy(way, f, k):
        first, count, _ = slabs[f]
        at = piece(f, k)
        landing = (left_t.at[pl.ds(first, count), at], right_t.at[pl.ds(first - coarse, count), at])[way]
        return remote(own_t.at[pl.ds(first, count), at], landing, send_z.at[way, peers - 1 + f, k],
                      recv_z.at[way, peers - 1 + f, k], (up, down)[way])

    def m_copy(way):
        return remote(moments, (left_moments, right_moments)[way], send_m.at[way],
                      recv_m.at[way], (up, down)[way])

    def each_way(action):
        for way, present in ((0, has_right), (1, has_left)):
            @pl.when(present)
            def _():
                action(way)

    def start_z(c):
        def go(way):
            for k in range(PARTS):
                z_copy(way, c, k).start()
        each_way(go)

    def start_t(f):
        def go(way):
            for k in range(slabs[f][2]):
                t_copy(way, f, k).start()
        each_way(go)

    start_z(0)

    @pl.when(jnp.logical_not(has_left))
    def _():
        left[...] = jnp.zeros_like(left)
        left_t[coarse:, :] = jnp.zeros((cut, rows), left_t.dtype)
        left_moments[...] = jnp.zeros_like(left_moments)

    @pl.when(jnp.logical_not(has_right))
    def _():
        right[...] = jnp.zeros_like(right)
        right_t[...] = jnp.zeros_like(right_t)
        right_moments[...] = jnp.zeros_like(right_moments)

    part0[...] = jnp.zeros_like(part0)
    part1[...] = jnp.zeros_like(part1)
    part2[...] = jnp.zeros_like(part2)
    last1[...] = jnp.zeros_like(last1)
    last_rows[...] = jnp.zeros_like(last_rows)
    last_columns[...] = jnp.zeros_like(last_columns)
    load.wait()

    step = 64

    def add_up(i, carry):
        s, q = carry
        v = own[pl.ds(pl.multiple_of(i * step, step), step), :].astype(jnp.float32)
        v = v.reshape(step // 8, 8, width)
        return s + jnp.sum(v, 0), q + jnp.sum(v * v, 0)

    zero = jnp.zeros((8, width), jnp.float32)
    s, q = lax.fori_loop(0, rows // step, add_up, (zero, zero))
    sums[0:1, :] = jnp.sum(s, 0, keepdims=True)
    sums[1:2, :] = jnp.sum(q, 0, keepdims=True)

    def s_copy(r):
        return remote(sums, stats.at[me], send_s.at[r], recv_s.at[me], {"samp": r})

    def s_from(j):
        return remote(sums, stats.at[j], send_s.at[j], recv_s.at[j], {"samp": j})

    def others(action):
        for r in range(peers):
            @pl.when(me != r)
            def _():
                action(r)

    others(lambda r: s_copy(r).start())
    stats[me] = sums[...]
    for copy in small:
        copy.wait()
    others(lambda r: s_from(r).wait_recv())
    both = stats[0]
    for j in range(1, peers):
        both = both + stats[j]
    mean = both[0:1] / samples
    var = both[1:2] / samples - mean * mean
    live = (lax.broadcasted_iota(jnp.int32, (1, width), 1) < counts[0]).astype(jnp.float32)
    keep = mask[...].astype(jnp.float32) * live
    moments[0:1, :] = mean
    moments[1:2, :] = lax.rsqrt(var + 1e-05) * keep
    each_way(lambda way: m_copy(way).start())
    for c in range(1, peers - 1):
        start_z(c)

    def standard(ref, at, which):
        v = ref[at].astype(jnp.float32)
        return (v - which[0:1, at[1]]) * which[1:2, at[1]]

    parts, pairs, fars = (part0, part1, part2), (pair0, pair1, pair2), (far0, far1, far2)

    def pair_copy(kind, c, r):
        columns, tall = columns_of(kind, c, r), height(kind, c, r)
        return remote(
            parts[kind].at[pl.ds(r * cut, tall), columns], pairs[kind].at[r // 2, pl.ds(0, tall), columns],
            send_a.at[kind, c, r // 2], recv_a.at[kind, c, r // 2], {"samp": me + 1 - 2 * odd})

    def far_copy(kind, c, r, source):
        columns, tall = columns_of(kind, c, r), pl.ds(0, height(kind, c, r))
        return remote(
            pairs[kind].at[r // 2, tall, columns], fars[kind].at[source, tall, columns],
            send_b.at[kind, c, r // 2], recv_b.at[kind, c, source], {"samp": r})

    def height(kind, c, r):
        return cut - fine if (kind, c, r) == (2, peers - 1, peers - 1) else cut

    def columns_of(kind, c, r):
        if kind == 0:
            return pl.ds(0, width)
        if kind == 1 or r < c:
            return pl.ds(c * cut, cut)
        return pl.ds(0, (c + 1) * cut)

    def takes(kind, c):
        return range(c + 1) if kind == 2 else range(peers)

    def send_pairs(kind, c, wait=False):
        for r in takes(kind, c):
            @pl.when(odd != r % 2)
            def _():
                copy = pair_copy(kind, c, r)
                copy.wait_send() if wait else copy.start()

    def sum_pairs(kind, c):
        for r in takes(kind, c):
            @pl.when(odd == r % 2)
            def _():
                columns, tall = columns_of(kind, c, r), height(kind, c, r)
                pair_copy(kind, c, r).wait_recv()
                pairs[kind][r // 2, :tall, columns] += parts[kind][pl.ds(r * cut, tall), columns]

                @pl.when(mine != r // 2)
                def _():
                    far_copy(kind, c, r, mine).start()

    def sent_pairs(kind, c):
        for r in takes(kind, c):
            @pl.when(jnp.logical_and(odd == r % 2, mine != r // 2))
            def _():
                far_copy(kind, c, r, mine).wait_send()

    def ship(c, r):
        at = pl.ds(0, height(2, c, r)), columns_of(2, c, r)
        return remote(total2.at[at], far.at[at], send_f.at[c], recv_f.at[c], down)

    def collect(kind, c):
        for r in takes(kind, c):
            @pl.when(me == r)
            def _():
                columns, tall = columns_of(kind, c, r), height(kind, c, r)
                whole = pairs[kind][r // 2, :tall, columns]
                for q in range(peers // 2):
                    if q != r // 2:
                        far_copy(kind, c, r, q).wait_recv()
                        whole = whole + fars[kind][q, :tall, columns]
                if kind < 2:
                    near[kind, :, columns] = whole
                else:
                    total2[:tall, columns] = whole.astype(total2.dtype)

    def start_ship(c):
        for r in takes(2, c):
            @pl.when(jnp.logical_and(me == r, has_left))
            def _():
                ship(c, r).start()

    def own_step(k, _):
        at = pl.ds(pl.multiple_of(k * deep, deep), deep)
        for c in range(peers):
            here = (at, pl.ds(c * cut, cut))
            z = standard(own, here, moments)
            own[here] = z.astype(jnp.bfloat16)
            own_t[pl.ds(c * cut, cut), at] = z.T.astype(jnp.bfloat16)
        part0[...] += jnp.dot(own_t[:, at], own[at, :], preferred_element_type=jnp.float32)
        return 0

    lax.fori_loop(0, PARTS, own_step, 0)
    send_pairs(0, 0)

    def wait_moments(way):
        m_copy(1 - way).wait_recv()

    each_way(wait_moments)

    def across(a, b):
        return lax.dot_general(a, b, (((1,), (1,)), ((), ())), preferred_element_type=jnp.float32)

    def along(a, b):
        return jnp.dot(a, b, preferred_element_type=jnp.float32)

    for c in range(peers - 1):
        def one(k, _, c=c):
            at, columns = here = block_of(c, k)
            earlier = ((2, c - 1), (1, c - 1)) if c else ((0, 0),)

            @pl.when(k == 1)
            def _():
                for which in earlier:
                    sum_pairs(*which)

            @pl.when(k == PARTS - 1)
            def _():
                for which in earlier:
                    collect(*which)

            @pl.when(has_left)
            def _():
                z_copy(0, c, k).wait_recv()

            z = standard(left, here, left_moments)
            left[here] = z.astype(jnp.bfloat16)
            left_t[columns, at] = z.T.astype(jnp.bfloat16)

            @pl.when(has_right)
            def _():
                z_copy(1, c, k).wait_recv()

            right[here] = standard(right, here, right_moments).astype(jnp.bfloat16)
            part1[:, columns] += along(own_t[:, at], right[here])
            top = pl.ds(0, (c + 1) * cut)
            part2[top, columns] += along(left_t[top, at], right[here])
            if c:
                front = pl.ds(0, c * cut)
                part2[columns, front] += along(left_t[columns, at], right[at, front])
            return 0

        lax.fori_loop(0, PARTS, one, 0)
        send_pairs(2, c)
        send_pairs(1, c)
        if c == 0:
            start_t(0)
            start_t(1)

    def wait_slab(f, k):
        @pl.when(has_left)
        def _():
            t_copy(0, f, k).wait_recv()

        @pl.when(has_right)
        def _():
            t_copy(1, f, k).wait_recv()

    whole_front, slab = pl.ds(0, coarse), pl.ds(coarse, cut - fine)

    def first_slab(k, _):
        at = piece(0, k)

        @pl.when(k == 1)
        def _():
            sum_pairs(2, peers - 2)
            sum_pairs(1, peers - 2)

        @pl.when(k == 2)
        def _():
            collect(2, peers - 2)
            for c in range(peers - 1):
                start_ship(c)
            collect(1, peers - 2)

        wait_slab(0, k)
        new = right_t[pl.ds(0, cut - fine), at]
        part1[:, slab] += across(own_t[:, at], new)
        part2[pl.ds(0, middle), slab] += across(left_t[pl.ds(0, middle), at], new)
        part2[slab, whole_front] += along(left_t[slab, at], right[at, :])
        return 0

    lax.fori_loop(0, PARTS, first_slab, 0)
    send_pairs(2, peers - 1)
    send_pairs(1, peers - 1)
    sum_pairs(2, peers - 1)

    def last_slab(k, _):
        at = piece(1, k)

        @pl.when(k == LAST_PARTS - 1)
        def _():
            sum_pairs(1, peers - 1)

        wait_slab(1, k)
        new = right_t[pl.ds(cut - fine, fine), at]
        last_columns[:, whole_front] += along(new, left[at, :])
        last_columns[:, slab] += across(new, left_t[slab, at])
        new_left = left_t[pl.ds(middle, fine), at]
        last_rows[:, whole_front] += along(new_left, right[at, :])
        last_rows[:, pl.ds(coarse, cut)] += across(new_left, right_t[:, at])
        last1[...] += along(new, own[at, :])
        return 0

    lax.fori_loop(0, LAST_PARTS, last_slab, 0)

    def columns_copy(r, source):
        return remote(out_columns.at[:, pl.ds(r * cut, cut)], land_columns.at[source],
                      send_c.at[r], recv_c.at[source], {"chain": m - 1, "samp": r})

    def rows_copy(source):
        return remote(out_rows, land_rows.at[source], send_r, recv_r.at[source],
                      {"chain": m - 1, "samp": peers - 1})

    def last1_copy(r, source):
        return remote(last1.at[:, pl.ds(r * cut, cut)], land1.at[source],
                      send_1.at[r], recv_1.at[source], {"samp": r})

    out_columns[...] = last_columns[...].astype(out_columns.dtype)
    out_rows[...] = last_rows[...].astype(out_rows.dtype)

    @pl.when(has_left)
    def _():
        rows_copy(me).start()
        for r in range(peers):
            columns_copy(r, me).start()

    others(lambda r: last1_copy(r, me).start())
    for r in range(peers):
        @pl.when(me == r)
        def _():
            land1[r] = last1[:, pl.ds(r * cut, cut)]

    collect(2, peers - 1)
    start_ship(peers - 1)
    collect(1, peers - 1)

    def turned(landed):
        total = landed[0].astype(jnp.float32)
        for j in range(1, peers):
            total = total + landed[j].astype(jnp.float32)
        return jnp.concatenate([jnp.zeros((cut - fine, cut), jnp.float32), total], 0).T

    others(lambda r: last1_copy(r, r).wait_recv())
    near[1, :, pl.ds(coarse, cut)] += turned(land1)

    @pl.when(jnp.logical_not(has_right))
    def _():
        near[2] = jnp.zeros_like(near[2])

    @pl.when(has_right)
    def _():
        for c in range(peers):
            for r in takes(2, c):
                @pl.when(me == r)
                def _():
                    ship(c, r).wait_recv()
        near[2, :cut - fine] = far[:cut - fine].astype(jnp.float32)

        @pl.when(me != peers - 1)
        def _():
            near[2, cut - fine:] = far[cut - fine:].astype(jnp.float32)

        @pl.when(me == peers - 1)
        def _():
            total = jnp.zeros((fine, width), jnp.float32)
            for source in range(peers):
                rows_copy(source).wait_recv()
                total = total + land_rows[source].astype(jnp.float32)
            near[2, cut - fine:] = total

        for source in range(peers):
            columns_copy(0, source).wait_recv()
        near[2, :, pl.ds(coarse, cut)] += turned(land_columns)

    @pl.when(has_left)
    def _():
        rows_copy(me).wait_send()
        for r in range(peers):
            columns_copy(r, me).wait_send()

    others(lambda r: last1_copy(r, me).wait_send())
    others(lambda r: s_copy(r).wait_send())
    each_way(lambda way: m_copy(way).wait_send())

    def sent(way):
        for k in range(PARTS):
            for c in range(peers - 1):
                z_copy(way, c, k).wait_send()
        for f in range(2):
            for k in range(slabs[f][2]):
                t_copy(way, f, k).wait_send()

    each_way(sent)
    for c in range(peers):
        for kind in (1, 2):
            send_pairs(kind, c, True)
            sent_pairs(kind, c)
        for r in takes(2, c):
            @pl.when(jnp.logical_and(me == r, has_left))
            def _():
                ship(c, r).wait_send()
    send_pairs(0, 0, True)
    sent_pairs(0, 0)


def body(n, peers, dosage, filter_mask, counts):
    rows, width = dosage.shape
    cut = width // peers
    fine = cut // FINE
    samples = rows * peers
    f32, bf16 = jnp.float32, jnp.bfloat16
    vmem = pl.BlockSpec(memory_space=pltpu.VMEM)
    dma = pltpu.SemaphoreType.DMA
    tiles = pl.pallas_call(
        functools.partial(kernel, n, peers, samples),
        out_shape=jax.ShapeDtypeStruct((3, cut, width), f32),
        in_specs=[pl.BlockSpec(memory_space=pl.ANY)] * 3,
        out_specs=vmem,
        scratch_shapes=[
            pltpu.VMEM((rows, width), bf16),
            *[pltpu.VMEM((rows, width - cut), bf16)] * 2,
            *[pltpu.VMEM((width, rows), bf16)] * 2,
            pltpu.VMEM((cut, rows), bf16),
            *[pltpu.VMEM((width, width), f32)] * 3,
            *[pltpu.VMEM((peers // 2, cut, width), f32)] * 6,
            pltpu.VMEM((2, width), f32),
            pltpu.VMEM((peers, 2, width), f32),
            *[pltpu.VMEM((2, width), f32)] * 3,
            *[pltpu.VMEM((cut, width), bf16)] * 2,
            *[pltpu.VMEM((fine, width), f32)] * 3,
            *[pltpu.VMEM((fine, width), bf16)] * 2,
            pltpu.VMEM((peers, fine, cut), f32),
            pltpu.VMEM((peers, fine, width), bf16),
            pltpu.VMEM((peers, fine, cut), bf16),
            pltpu.VMEM((1, width), jnp.int32),
            pltpu.SMEM((1,), jnp.int32),
            *[dma] * 3,
            *[dma((2, peers + 1, max(PARTS, LAST_PARTS)))] * 2,
            *[dma((2,))] * 2,
            *[dma((peers,))] * 2,
            *[dma((3, peers, peers // 2))] * 4,
            *[dma((peers,))] * 2,
            *[dma((peers,))] * 2,
            dma, dma((peers,)),
            *[dma((peers,))] * 2,
        ],
        compiler_params=pltpu.CompilerParams(
            collective_id=0, has_side_effects=True, vmem_limit_bytes=52 * 2**20),
    )(*[pltpu.with_memory_space_constraint(a, pltpu.HBM) for a in (dosage, filter_mask[None])], counts)
    return jnp.transpose(tiles / samples, (1, 0, 2))[None]


def solution(mesh):
    in_specs = (P("samp", ("groups", "chain")), P(("groups", "chain")), P(("groups", "chain")))
    out_specs = P(("groups", "chain"), "samp", None, None)
    run = functools.partial(body, mesh.shape["chain"], mesh.shape["samp"])
    return jax.shard_map(run, mesh=mesh, in_specs=in_specs, out_specs=out_specs, check_vma=False)
```
